32 devices in a mesh: row: 16 (over z, y, core), vec: 2 (over x).
Axes of the slice: x: 2, y: 2, z: 4, core: 2. Of those that a mesh axis runs over, the one named last changes fastest.
Arguments:
- eigvecs: float32 [8192, 2048], P('row', 'vec'), may hold values from -6 to 6
- reflectors: float32 [6, 8192, 128], P(None, 'row', 'vec'), may hold values from -0.375 to 0.375
- factors: float32 [6, 32, 128, 128], P(None, 'row', 'vec'), may hold values from -0.25 to 0.25
Outputs:
- vectors: float32 [8192, 2048], P('row', 'vec')
The draws below stay inside these ranges and needn't reach their ends.
All inputs are finite; a program needn't handle non-finite values.
Results may differ from the reference program's by a relative error of at most 0.0001.
Values sent between devices are 32-bit elements; how exact they have to be, the bound alone decides.
A program may use at most 64 MiB of HBM per device.

```python
import jax
import jax.numpy as jnp
from jax import lax

NB = 128
ROUNDS = 6
ROWS = 8192
COLS = 2048
GROUPS = 32


def steps_of(rng, shape, pieces, smallest, high):
    factor_of = 1.0
    for position, shards_of in pieces:
        heights = jax.random.uniform(jax.random.fold_in(jax.random.fold_in(rng, 6), position), (shards_of,), jnp.float32, smallest / len(pieces), high / len(pieces))
        factor_of = factor_of * jnp.repeat(jnp.exp(heights), shape[position] // shards_of).reshape((-1,) + (1,) * (len(shape) - 1 - position))
    return factor_of


def noise(own_key, shape, deviation, bound, cuts=(), held_as=jnp.bfloat16):
    array = deviation * jax.random.normal(own_key, shape, jnp.float32)
    if cuts:
        array = array * steps_of(own_key, shape, cuts, -0.22, 0.18)
    return jnp.clip(array, -bound, bound).astype(held_as)


def setup_inputs(seed: int = 0) -> dict:
    key_list = jax.random.split(jax.random.key(seed), 4)
    return {
        "eigvecs": noise(key_list[0], (ROWS, COLS), 1.0, 6.0, ((0, 16), (1, 2)), jnp.float32),
        "reflectors": noise(key_list[1], (ROUNDS, ROWS, NB), (2 * NB) ** -0.5, 0.375, ((1, 16), (2, 2)), jnp.float32),
        "factors": noise(key_list[2], (ROUNDS, GROUPS, NB, NB), (4 * NB) ** -0.5, 0.25, ((1, 16), (2, 2)), jnp.float32),
    }


highest = lax.Precision.HIGHEST


def apply_groups(panel, basis, blocks):
    inner = jnp.einsum('gri,grc->gic', basis, panel, precision=highest)
    images = jnp.einsum('gij,gjc->gic', blocks, inner, precision=highest)
    return panel - jnp.einsum('gri,gic->grc', basis, images, precision=highest)


def reference(eigvecs, reflectors, factors):
    vectors = eigvecs
    total = vectors.shape[0]
    width = vectors.shape[1]
    for number in range(ROUNDS):
        offset = number * NB
        count = (total - offset + 2 * NB - 1) // (2 * NB)
        filler = count * 2 * NB - (total - offset)
        panel = jnp.pad(vectors[offset:], ((0, filler), (0, 0))).reshape(count, 2 * NB, width)
        basis = jnp.pad(reflectors[number, offset:], ((0, filler), (0, 0))).reshape(count, 2 * NB, NB)
        panel = apply_groups(panel, basis, factors[number, :count])
        vectors = jnp.concatenate([vectors[:offset], panel.reshape(count * 2 * NB, width)[:total - offset]], 0)
    return vectors
```

```python
import functools

import jax
import jax.numpy as jnp
from jax import lax
from jax.experimental import pallas as pl
from jax.experimental.pallas import tpu as pltpu
from jax.sharding import PartitionSpec as P

MESH = pl.DeviceIdType.MESH
CHUNKS = 4


def split(value):
    high = value.astype(jnp.bfloat16)
    return high, (value - high.astype(jnp.float32)).astype(jnp.bfloat16)


def dot(left, right):
    return lax.dot_general(
        left, right, (((1,), (0,)), ((), ())),
        precision=lax.Precision.DEFAULT, preferred_element_type=jnp.float32,
    )


def kernel(
    count, peers, eig, refl, fact, out,
    x, vown, vt, tall, vcat, ucat, wsend, wrecv,
    xin, vin, vsend, vrecv, tsend, trecv, wss, wrs, xout,
):
    rounds, height, share = vown.shape
    nb = vt.shape[1]
    groups = height // (2 * nb)
    chunks, _, wide = x.shape
    d = lax.axis_index("row")
    v = lax.axis_index("vec")

    def peer(o):
        return lax.rem(v + o, peers)

    def rows_of(p):
        return pl.ds(pl.multiple_of(p * share, 8), share)

    def slots(r):
        for k in range(-1 if r % 2 else 0, groups):
            q = k - r // 2
            yield k + 1, q % groups, -(q // groups)

    reach = max(away for r in range(rounds) for _, _, away in slots(r))

    for r in range(rounds):
        pltpu.make_async_copy(refl.at[r], vown.at[r], vin.at[r]).start()
    for c in range(chunks):
        pltpu.make_async_copy(eig.at[:, pl.ds(c * wide, wide)], x.at[c], xin.at[c]).start()

    barrier = pltpu.get_barrier_semaphore()
    valid = jnp.int32(0)
    for away in range(-reach, reach + 1):
        inside = jnp.logical_and(d + away >= 0, d + away < count)
        valid = valid + inside.astype(jnp.int32)

        @pl.when(inside)
        def _():
            for o in range(peers):
                if away != 0 or o != 0:
                    pl.semaphore_signal(
                        barrier, inc=1, device_id=(d + away, peer(o)), device_id_type=MESH
                    )

    pl.semaphore_wait(barrier, valid * peers - 1)

    def t_copy(r, slot, source, away, o):
        return pltpu.make_async_remote_copy(
            src_ref=fact.at[r, source],
            dst_ref=tall.at[r, slot, rows_of(v)],
            send_sem=tsend.at[r, slot, o],
            recv_sem=trecv.at[r, slot],
            device_id=(d + away, peer(o)),
            device_id_type=MESH,
        )

    def v_copy(r, o):
        return pltpu.make_async_remote_copy(
            src_ref=vt.at[r, rows_of(v)],
            dst_ref=vt.at[r, rows_of(v)],
            send_sem=vsend.at[r, o - 1],
            recv_sem=vrecv.at[r, o - 1],
            device_id=(d, peer(o)),
            device_id_type=MESH,
        )

    for r in range(rounds):
        pltpu.make_async_copy(refl.at[r], vown.at[r], vin.at[r]).wait()
        vt[r, rows_of(v)] = jnp.transpose(vown[r])
        for o in range(1, peers):
            v_copy(r, o).start()
        for slot, source, away in slots(r):
            for o in range(peers):
                if away == 0 and o == 0:
                    pltpu.make_async_copy(
                        fact.at[r, source], tall.at[r, slot, rows_of(v)], trecv.at[r, slot]
                    ).start()
                elif away == 0:
                    t_copy(r, slot, source, away, o).start()
                else:
                    @pl.when(d + away < count)
                    def _():
                        t_copy(r, slot, source, away, o).start()

    @pl.when(d == 0)
    def _():
        wrecv[:, 0] = jnp.zeros((rounds // 2, chunks, nb, wide), jnp.float32)

    @pl.when(d == count - 1)
    def _():
        wrecv[:, 1] = jnp.zeros((rounds // 2, chunks, nb, wide), jnp.float32)

    def prepare_v(r):
        for o in range(1, peers):
            part = vt.at[r, rows_of(lax.rem(v + peers - o, peers))]
            pltpu.make_async_copy(part, part, vrecv.at[r, o - 1]).wait()
        vcat[r, :nb], vcat[r, nb:] = split(vt[r])

    def prepare_u(r):
        for slot, _, away in slots(r):
            whole = tall.at[r, slot]
            arrived = pltpu.make_async_copy(whole, whole, trecv.at[r, slot])
            if away == 0:
                arrived.wait()
            else:
                @pl.when(d >= away)
                def _():
                    arrived.wait()

                @pl.when(d < away)
                def _():
                    tall[r, slot] = jnp.zeros((nb, nb), jnp.float32)

            first = (slot - 1) * 2 * nb + (r % 2) * nb
            begin, end = max(first, 0), min(first + 2 * nb, height)
            bh, bl = split(jnp.transpose(vt[r, :, begin:end]))
            th, tl = split(tall[r, slot])
            uh, ul = split(dot(bh, th) + dot(bh, tl) + dot(bl, th))
            ucat[r, begin:end, :nb] = uh
            ucat[r, begin:end, nb : 2 * nb] = ul
            ucat[r, begin:end, 2 * nb :] = uh

    def inner(r, c, begin, end):
        xh, xl = split(x[c, begin:end])
        both = dot(vcat[r, :, begin:end], xh)
        return both[:nb] + both[nb:] + dot(vcat[r, :nb, begin:end], xl)

    def update(r, c, begin, end, w):
        wh, wl = split(w)
        stacked = jnp.concatenate([wh, wh, wl], 0)
        x[c, begin:end] = x[c, begin:end] - dot(ucat[r, begin:end], stacked)

    def even(r, c):
        for g in range(groups):
            begin, end = 2 * nb * g, 2 * nb * (g + 1)
            update(r, c, begin, end, inner(r, c, begin, end))

    def middle(r, c):
        for g in range(groups - 1):
            begin, end = 2 * nb * g + nb, 2 * nb * (g + 1) + nb
            update(r, c, begin, end, inner(r, c, begin, end))

    sides = ((0, nb), (height - nb, height))

    def w_copy(r, c, side):
        return pltpu.make_async_remote_copy(
            src_ref=wsend.at[r // 2, side, c],
            dst_ref=wrecv.at[r // 2, 1 - side, c],
            send_sem=wss.at[r // 2, side, c],
            recv_sem=wrs.at[r // 2, 1 - side, c],
            device_id=(d + 2 * side - 1, v),
            device_id_type=MESH,
        )

    has = (d > 0, d < count - 1)

    def before(r, c):
        for side in (0, 1):
            wsend[r // 2, side, c] = inner(r, c, *sides[side])

            @pl.when(has[side])
            def _():
                w_copy(r, c, side).start()

    def after(r, c):
        for side in (0, 1):
            landed = wrecv.at[r // 2, side, c]

            @pl.when(has[side])
            def _():
                pltpu.make_async_copy(landed, landed, wrs.at[r // 2, side, c]).wait()

            update(r, c, *sides[side], wsend[r // 2, side, c] + wrecv[r // 2, side, c])

    def over_chunks(body):
        lax.fori_loop(0, chunks, lambda c, carry: (body(c), carry)[1], 0)

    prepare_v(0)
    prepare_u(0)
    prepare_v(1)
    for c in range(chunks):
        pltpu.make_async_copy(eig.at[:, pl.ds(c * wide, wide)], x.at[c], xin.at[c]).wait()

    for r in range(1, rounds, 2):
        def step(c):
            if r > 1:
                after(r - 2, c)
            even(r - 1, c)
            before(r, c)

        over_chunks(step)
        prepare_u(r)
        over_chunks(lambda c: middle(r, c))
        if r + 2 < rounds:
            prepare_v(r + 1)
            prepare_u(r + 1)
            prepare_v(r + 2)

    def store(c):
        return pltpu.make_async_copy(
            x.at[c], out.at[:, pl.ds(pl.multiple_of(c * wide, wide), wide)], xout.at[c]
        )

    def finish(c):
        after(rounds - 1, c)
        store(c).start()

    over_chunks(finish)

    for r in range(rounds):
        for o in range(1, peers):
            v_copy(r, o).wait_send()
        for slot, source, away in slots(r):
            for o in range(peers):
                if away == 0 and o != 0:
                    t_copy(r, slot, source, away, o).wait_send()
                elif away != 0:
                    @pl.when(d + away < count)
                    def _():
                        t_copy(r, slot, source, away, o).wait_send()

    for side in (0, 1):
        @pl.when(has[side])
        def _():
            for r in range(1, rounds, 2):
                over_chunks(lambda c: w_copy(r, c, side).wait_send())

    over_chunks(lambda c: store(c).wait())


def solution(mesh):
    count, peers = mesh.shape["row"], mesh.shape["vec"]

    def per_device(eigvecs, reflectors, factors):
        height, width = eigvecs.shape
        rounds, _, share = reflectors.shape
        nb = factors.shape[3]
        groups = height // (2 * nb)
        wide = width // CHUNKS
        f32, bf16, dma = jnp.float32, jnp.bfloat16, pltpu.SemaphoreType.DMA
        links = (rounds // 2, 2, CHUNKS)
        return pl.pallas_call(
            functools.partial(kernel, count, peers),
            out_shape=jax.ShapeDtypeStruct((height, width), f32),
            in_specs=[pl.BlockSpec(memory_space=pl.ANY)] * 3,
            out_specs=pl.BlockSpec(memory_space=pl.ANY),
            scratch_shapes=[
                pltpu.VMEM((CHUNKS, height, wide), f32),
                pltpu.VMEM((rounds, height, share), f32),
                pltpu.VMEM((rounds, nb, height), f32),
                pltpu.VMEM((rounds, groups + 1, nb, nb), f32),
                pltpu.VMEM((rounds, 2 * nb, height), bf16),
                pltpu.VMEM((rounds, height, 3 * nb), bf16),
                pltpu.VMEM(links + (nb, wide), f32),
                pltpu.VMEM(links + (nb, wide), f32),
                dma((CHUNKS,)),
                dma((rounds,)),
                dma((rounds, peers - 1)),
                dma((rounds, peers - 1)),
                dma((rounds, groups + 1, peers)),
                dma((rounds, groups + 1)),
                dma(links),
                dma(links),
                dma((CHUNKS,)),
            ],
            compiler_params=pltpu.CompilerParams(
                collective_id=0, has_side_effects=True, vmem_limit_bytes=48 << 20
            ),
            name="back_transform",
        )(eigvecs, reflectors, factors)

    return jax.shard_map(
        per_device,
        mesh=mesh,
        in_specs=(P("row", "vec"), P(None, "row", "vec"), P(None, "row", "vec", None)),
        out_specs=P("row", "vec"),
        check_vma=False,
    )
```

```python
import functools

import jax
import jax.numpy as jnp
from jax import lax
from jax.experimental import pallas as pl
from jax.experimental.pallas import tpu as pltpu
from jax.sharding import PartitionSpec as P

MESH = pl.DeviceIdType.MESH
CHUNKS = 4


def split(value):
    high = value.astype(jnp.bfloat16)
    return high, (value - high.astype(jnp.float32)).astype(jnp.bfloat16)


def dot(left, right):
    return lax.dot_general(
        left, right, (((1,), (0,)), ((), ())),
        precision=lax.Precision.DEFAULT, preferred_element_type=jnp.float32,
    )


def kernel(
    count, peers, eig, refl, fact, out,
    x, vt, tall, vcat, ucat, wsend, wrecv,
    xin, vsend, vrecv, tsend, trecv, wss, wrs, xout,
):
    rounds, nb, height = vt.shape
    share = refl.shape[1]
    groups = height // (2 * nb)
    chunks, _, wide = x.shape
    d = lax.axis_index("row")
    v = lax.axis_index("vec")
    odd = lax.rem(d, 2)

    def peer(o):
        return lax.rem(v + o, peers)

    def rows_of(p):
        return pl.ds(pl.multiple_of(p * share, 8), share)

    def turn(i, last):
        return i + odd * (last - 2 * i)

    def group_rows(i):
        return pl.ds(pl.multiple_of(turn(i, groups - 1) * 2 * nb, nb), 2 * nb)

    def side_rows(i):
        return pl.ds(pl.multiple_of(turn(i, 1) * (height - nb), nb), nb)

    def middle_rows(g):
        return pl.ds(2 * nb * g + nb, 2 * nb)

    def pieces(r):
        if r == 0:
            return [group_rows(i) for i in range(groups)]
        if r == 1:
            return [side_rows(0), side_rows(1)] + [pl.ds(nb, height - 2 * nb)]
        return [pl.ds(0, height)]

    def slots(r):
        for k in range(-1 if r % 2 else 0, groups):
            q = k - r // 2
            yield k + 1, q % groups, -(q // groups)

    reach = max(away for r in range(rounds) for _, _, away in slots(r))

    def load(c):
        return pltpu.make_async_copy(eig.at[:, pl.ds(c * wide, wide)], x.at[c], xin.at[c])

    barrier = pltpu.get_barrier_semaphore()
    valid = jnp.int32(0)
    for away in range(-reach, reach + 1):
        inside = jnp.logical_and(d + away >= 0, d + away < count)
        valid = valid + inside.astype(jnp.int32)

        @pl.when(inside)
        def _():
            for o in range(peers):
                if away != 0 or o != 0:
                    pl.semaphore_signal(
                        barrier, inc=1, device_id=(d + away, peer(o)), device_id_type=MESH
                    )

    for c in range(chunks):
        load(c).start()
    pl.semaphore_wait(barrier, valid * peers - 1)

    def t_copy(r, slot, source, away, o):
        return pltpu.make_async_remote_copy(
            src_ref=fact.at[r, source],
            dst_ref=tall.at[r, slot, rows_of(v)],
            send_sem=tsend.at[r, slot, o],
            recv_sem=trecv.at[r, slot],
            device_id=(d + away, peer(o)),
            device_id_type=MESH,
        )

    def v_copy(r, piece, where, o):
        return pltpu.make_async_remote_copy(
            src_ref=refl.at[r, :, where],
            dst_ref=vt.at[r, rows_of(v), where],
            send_sem=vsend.at[r, piece, o],
            recv_sem=vrecv.at[r, piece, o],
            device_id=(d, peer(o)),
            device_id_type=MESH,
        )

    def send_v(r, piece):
        where = pieces(r)[piece]
        for o in range(1, peers):
            v_copy(r, piece, where, o).start()
        pltpu.make_async_copy(
            refl.at[r, :, where], vt.at[r, rows_of(v), where], vrecv.at[r, piece, 0]
        ).start()

    def send_t(r, slot, source, away):
        for o in range(peers):
            if not isinstance(away, int) or away != 0:
                @pl.when(d + away < count)
                def _():
                    t_copy(r, slot, source, away, o).start()
            elif o != 0:
                t_copy(r, slot, source, away, o).start()
            else:
                pltpu.make_async_copy(
                    fact.at[r, source], tall.at[r, slot, rows_of(v)], trecv.at[r, slot]
                ).start()

    def send_round(r):
        for piece in range(len(pieces(r))):
            send_v(r, piece)
        for entry in slots(r):
            send_t(r, *entry)

    for i in range(groups):
        g = turn(i, groups - 1)
        send_v(0, i)
        send_t(0, g + 1, g, 0)
        if i == 0:
            send_v(1, 0)
    send_v(1, 1)
    send_v(1, 2)
    for entry in slots(1):
        send_t(1, *entry)

    @pl.when(d == 0)
    def _():
        wrecv[:, 0] = jnp.zeros((rounds // 2, chunks, nb, wide), jnp.float32)

    @pl.when(d == count - 1)
    def _():
        wrecv[:, 1] = jnp.zeros((rounds // 2, chunks, nb, wide), jnp.float32)

    def prepare_v(r, piece):
        where = pieces(r)[piece]
        for o in range(peers):
            part = vt.at[r, rows_of(lax.rem(v + peers - o, peers)), where]
            pltpu.make_async_copy(part, part, vrecv.at[r, piece, o]).wait()
        high, low = split(vt[r, :, where])
        vcat[r, :nb, where] = high
        vcat[r, nb:, where] = low

    def form_u(r, slot, where):
        bh, bl = split(jnp.transpose(vt[r, :, where]))
        th, tl = split(tall[r, slot])
        uh, ul = split(dot(bh, th) + dot(bh, tl) + dot(bl, th))
        ucat[r, where, :nb] = uh
        ucat[r, where, nb : 2 * nb] = ul
        ucat[r, where, 2 * nb :] = uh

    def arrived(r, slot):
        whole = tall.at[r, slot]
        return pltpu.make_async_copy(whole, whole, trecv.at[r, slot])

    def prepare_u(r):
        for slot, _, away in slots(r):
            if away == 0:
                arrived(r, slot).wait()
            else:
                @pl.when(d >= away)
                def _():
                    arrived(r, slot).wait()

                @pl.when(d < away)
                def _():
                    tall[r, slot] = jnp.zeros((nb, nb), jnp.float32)

            first = (slot - 1) * 2 * nb + (r % 2) * nb
            begin, end = max(first, 0), min(first + 2 * nb, height)
            form_u(r, slot, pl.ds(begin, end - begin))

    def inner(r, c, rows):
        xh, xl = split(x[c, rows])
        both = dot(vcat[r, :, rows], xh)
        return both[:nb] + both[nb:] + dot(vcat[r, :nb, rows], xl)

    def update(r, c, rows, w):
        wh, wl = split(w)
        stacked = jnp.concatenate([wh, wh, wl], 0)
        x[c, rows] = x[c, rows] - dot(ucat[r, rows], stacked)

    def apply(r, c, rows):
        update(r, c, rows, inner(r, c, rows))

    def middle(r, c):
        for g in range(groups - 1):
            apply(r, c, middle_rows(g))

    def neighbour(i):
        return d + 2 * turn(i, 1) - 1

    def reachable(i):
        return jnp.logical_and(neighbour(i) >= 0, neighbour(i) < count)

    def w_copy(r, c, i):
        side = turn(i, 1)
        return pltpu.make_async_remote_copy(
            src_ref=wsend.at[r // 2, side, c],
            dst_ref=wrecv.at[r // 2, 1 - side, c],
            send_sem=wss.at[r // 2, side, c],
            recv_sem=wrs.at[r // 2, 1 - side, c],
            device_id=(neighbour(i), v),
            device_id_type=MESH,
        )

    def before(r, c, i):
        wsend[r // 2, turn(i, 1), c] = inner(r, c, side_rows(i))

        @pl.when(reachable(i))
        def _():
            w_copy(r, c, i).start()

    def after(r, c, i):
        side = turn(i, 1)
        landed = wrecv.at[r // 2, side, c]

        @pl.when(reachable(i))
        def _():
            pltpu.make_async_copy(landed, landed, wrs.at[r // 2, side, c]).wait()

        update(r, c, side_rows(i), wsend[r // 2, side, c] + wrecv[r // 2, side, c])

    def over_chunks(body):
        lax.fori_loop(0, chunks, lambda c, carry: (body(c), carry)[1], 0)

    for i in range(groups):
        g = turn(i, groups - 1)
        prepare_v(0, i)
        if i == 0:
            for r in range(2, rounds, 2):
                send_round(r)
                send_round(r + 1)
        arrived(0, g + 1).wait()
        form_u(0, g + 1, group_rows(i))
        if i == 0:
            for c in range(chunks):
                load(c).wait()
        over_chunks(lambda c: apply(0, c, group_rows(i)))
        if i == 0:
            prepare_v(1, 0)
            over_chunks(lambda c: before(1, c, 0))
    prepare_v(1, 1)
    over_chunks(lambda c: before(1, c, 1))
    prepare_v(1, 2)
    prepare_u(1)
    over_chunks(lambda c: middle(1, c))

    for r in range(2, rounds, 2):
        prepare_v(r, 0)
        prepare_u(r)
        prepare_v(r + 1, 0)

        def step(c):
            for i in range(groups):
                if i < 2:
                    after(r - 1, c, i)
                apply(r, c, group_rows(i))
                if i == 0:
                    before(r + 1, c, 0)
            before(r + 1, c, 1)

        over_chunks(step)
        prepare_u(r + 1)
        over_chunks(lambda c: middle(r + 1, c))

    def store(c):
        return pltpu.make_async_copy(
            x.at[c], out.at[:, pl.ds(pl.multiple_of(c * wide, wide), wide)], xout.at[c]
        )

    def finish(c):
        after(rounds - 1, c, 0)
        after(rounds - 1, c, 1)
        store(c).start()

    over_chunks(finish)

    for r in range(rounds):
        for piece, where in enumerate(pieces(r)):
            for o in range(1, peers):
                v_copy(r, piece, where, o).wait_send()
        for slot, source, away in slots(r):
            for o in range(peers):
                if away == 0 and o != 0:
                    t_copy(r, slot, source, away, o).wait_send()
                elif away != 0:
                    @pl.when(d + away < count)
                    def _():
                        t_copy(r, slot, source, away, o).wait_send()

    for i in (0, 1):
        @pl.when(reachable(i))
        def _():
            for r in range(1, rounds, 2):
                over_chunks(lambda c: w_copy(r, c, i).wait_send())

    over_chunks(lambda c: store(c).wait())


def solution(mesh):
    count, peers = mesh.shape["row"], mesh.shape["vec"]

    def per_device(eigvecs, reflectors, factors):
        height, width = eigvecs.shape
        rounds = reflectors.shape[0]
        nb = factors.shape[3]
        groups = height // (2 * nb)
        wide = width // CHUNKS
        f32, bf16, dma = jnp.float32, jnp.bfloat16, pltpu.SemaphoreType.DMA
        links = (rounds // 2, 2, CHUNKS)
        return pl.pallas_call(
            functools.partial(kernel, count, peers),
            out_shape=jax.ShapeDtypeStruct((height, width), f32),
            in_specs=[pl.BlockSpec(memory_space=pltpu.HBM)] * 3,
            out_specs=pl.BlockSpec(memory_space=pl.ANY),
            scratch_shapes=[
                pltpu.VMEM((CHUNKS, height, wide), f32),
                pltpu.VMEM((rounds, nb, height), f32),
                pltpu.VMEM((rounds, groups + 1, nb, nb), f32),
                pltpu.VMEM((rounds, 2 * nb, height), bf16),
                pltpu.VMEM((rounds, height, 3 * nb), bf16),
                pltpu.VMEM(links + (nb, wide), f32),
                pltpu.VMEM(links + (nb, wide), f32),
                dma((CHUNKS,)),
                dma((rounds, 3, peers)),
                dma((rounds, 3, peers)),
                dma((rounds, groups + 1, peers)),
                dma((rounds, groups + 1)),
                dma(links),
                dma(links),
                dma((CHUNKS,)),
            ],
            compiler_params=pltpu.CompilerParams(
                collective_id=0, has_side_effects=True, vmem_limit_bytes=64500000
            ),
            name="back_transform",
        )(eigvecs, jnp.transpose(reflectors, (0, 2, 1)), factors)

    return jax.shard_map(
        per_device,
        mesh=mesh,
        in_specs=(P("row", "vec"), P(None, "row", "vec"), P(None, "row", "vec", None)),
        out_specs=P("row", "vec"),
        check_vma=False,
    )
```

```python
import functools

import jax
import jax.numpy as jnp
from jax import lax
from jax.experimental import pallas as pl
from jax.experimental.pallas import tpu as pltpu
from jax.sharding import PartitionSpec as P

MESH = pl.DeviceIdType.MESH
CHUNKS = 4


def split(value):
    high = value.astype(jnp.bfloat16)
    return high, (value - high.astype(jnp.float32)).astype(jnp.bfloat16)


def dot(left, right):
    return lax.dot_general(
        left, right, (((1,), (0,)), ((), ())),
        precision=lax.Precision.DEFAULT, preferred_element_type=jnp.float32,
    )


def kernel(
    count, peers, eig, refl, fact, out,
    x, vt, tall, vcat, ucat, wsend, wrecv,
    xin, vsend, vrecv, tsend, trecv, wss, wrs, xout,
):
    rounds, nb, height = vt.shape
    share = refl.shape[1]
    groups = height // (2 * nb)
    chunks, _, wide = x.shape
    d = lax.axis_index("row")
    v = lax.axis_index("vec")
    odd = lax.rem(d, 2)

    def peer(o):
        return lax.rem(v + o, peers)

    def rows_of(p):
        return pl.ds(pl.multiple_of(p * share, 8), share)

    def turn(i, last):
        return i + odd * (last - 2 * i)

    def group_rows(i):
        return pl.ds(pl.multiple_of(turn(i, groups - 1) * 2 * nb, nb), 2 * nb)

    def side_rows(i):
        return pl.ds(pl.multiple_of(turn(i, 1) * (height - nb), nb), nb)

    def middle_rows(g):
        return pl.ds(2 * nb * g + nb, 2 * nb)

    def pieces(r):
        if r == 0:
            return [group_rows(i) for i in range(groups)]
        if r == 1:
            return [side_rows(0), side_rows(1)] + [pl.ds(nb, height - 2 * nb)]
        return [pl.ds(0, height)]

    def slots(r):
        for k in range(-1 if r % 2 else 0, groups):
            q = k - r // 2
            yield k + 1, q % groups, -(q // groups)

    reach = max(away for r in range(rounds) for _, _, away in slots(r))

    def load(c):
        return pltpu.make_async_copy(eig.at[:, pl.ds(c * wide, wide)], x.at[c], xin.at[c])

    barrier = pltpu.get_barrier_semaphore()
    valid = jnp.int32(0)
    for away in range(-reach, reach + 1):
        inside = jnp.logical_and(d + away >= 0, d + away < count)
        valid = valid + inside.astype(jnp.int32)

        @pl.when(inside)
        def _():
            for o in range(peers):
                if away != 0 or o != 0:
                    pl.semaphore_signal(
                        barrier, inc=1, device_id=(d + away, peer(o)), device_id_type=MESH
                    )

    for c in range(chunks):
        load(c).start()
    pl.semaphore_wait(barrier, valid * peers - 1)

    def t_copy(r, slot, source, away, o):
        mine = tall.at[r, slot, rows_of(v)]
        return pltpu.make_async_remote_copy(
            src_ref=fact.at[r, source] if o == 0 or away == 0 else mine,
            dst_ref=mine,
            send_sem=tsend.at[r, slot, o],
            recv_sem=trecv.at[r, slot, o],
            device_id=(d + away if o == 0 else d, peer(o)),
            device_id_type=MESH,
        )

    def v_copy(r, piece, where, o):
        return pltpu.make_async_remote_copy(
            src_ref=refl.at[r, :, where],
            dst_ref=vt.at[r, rows_of(v), where],
            send_sem=vsend.at[r, piece, o],
            recv_sem=vrecv.at[r, piece, o],
            device_id=(d, peer(o)),
            device_id_type=MESH,
        )

    def send_v(r, piece):
        where = pieces(r)[piece]
        for o in range(1, peers):
            v_copy(r, piece, where, o).start()
        pltpu.make_async_copy(
            refl.at[r, :, where], vt.at[r, rows_of(v), where], vrecv.at[r, piece, 0]
        ).start()

    def own_t(r, slot, source):
        return pltpu.make_async_copy(
            fact.at[r, source], tall.at[r, slot, rows_of(v)], trecv.at[r, slot, 0]
        )

    def landed_t(r, slot, o):
        part = tall.at[r, slot, rows_of(lax.rem(v + peers - o, peers))]
        return pltpu.make_async_copy(part, part, trecv.at[r, slot, o])

    def send_t(r, slot, source, away):
        if away == 0:
            own_t(r, slot, source).start()
            for o in range(1, peers):
                t_copy(r, slot, source, away, o).start()
        else:
            @pl.when(d >= away)
            def _():
                landed_t(r, slot, 0).wait()
                for o in range(1, peers):
                    t_copy(r, slot, source, away, o).start()

    def send_round(r):
        for piece in range(len(pieces(r))):
            send_v(r, piece)
        for entry in slots(r):
            send_t(r, *entry)

    send_v(0, 0)
    for r in range(rounds):
        for slot, source, away in slots(r):
            if away != 0:
                @pl.when(d + away < count)
                def _():
                    t_copy(r, slot, source, away, 0).start()
    for i in range(groups):
        g = turn(i, groups - 1)
        if i > 0:
            send_v(0, i)
        send_t(0, g + 1, g, 0)
        if i == 0:
            send_v(1, 0)
    send_v(1, 1)
    send_v(1, 2)

    @pl.when(d == 0)
    def _():
        wrecv[:, 0] = jnp.zeros((rounds // 2, chunks, nb, wide), jnp.float32)

    @pl.when(d == count - 1)
    def _():
        wrecv[:, 1] = jnp.zeros((rounds // 2, chunks, nb, wide), jnp.float32)

    def prepare_v(r, piece):
        where = pieces(r)[piece]
        for o in range(peers):
            part = vt.at[r, rows_of(lax.rem(v + peers - o, peers)), where]
            pltpu.make_async_copy(part, part, vrecv.at[r, piece, o]).wait()
        high, low = split(vt[r, :, where])
        vcat[r, :nb, where] = high
        vcat[r, nb:, where] = low

    def form_u(r, slot, where):
        bh, bl = split(jnp.transpose(vt[r, :, where]))
        th, tl = split(tall[r, slot])
        uh, ul = split(dot(bh, th) + dot(bh, tl) + dot(bl, th))
        ucat[r, where, :nb] = uh
        ucat[r, where, nb : 2 * nb] = ul
        ucat[r, where, 2 * nb :] = uh

    def arrived(r, slot, away):
        for o in range(0 if away == 0 else 1, peers):
            landed_t(r, slot, o).wait()

    def prepare_u(r):
        for slot, _, away in slots(r):
            if away == 0:
                arrived(r, slot, away)
            else:
                @pl.when(d >= away)
                def _():
                    arrived(r, slot, away)

                @pl.when(d < away)
                def _():
                    tall[r, slot] = jnp.zeros((nb, nb), jnp.float32)

            first = (slot - 1) * 2 * nb + (r % 2) * nb
            begin, end = max(first, 0), min(first + 2 * nb, height)
            form_u(r, slot, pl.ds(begin, end - begin))

    def inner(r, rows, value):
        xh, xl = split(value)
        both = dot(vcat[r, :, rows], xh)
        return both[:nb] + both[nb:] + dot(vcat[r, :nb, rows], xl)

    def updated(r, rows, value, w):
        wh, wl = split(w)
        stacked = jnp.concatenate([wh, wh, wl], 0)
        return value - dot(ucat[r, rows], stacked)

    def apply(r, c, rows):
        value = x[c, rows]
        x[c, rows] = updated(r, rows, value, inner(r, rows, value))

    def middle(r, c):
        for g in range(groups - 1):
            apply(r, c, middle_rows(g))

    def neighbour(i):
        return d + 2 * turn(i, 1) - 1

    def reachable(i):
        return jnp.logical_and(neighbour(i) >= 0, neighbour(i) < count)

    def w_copy(r, c, i):
        side = turn(i, 1)
        return pltpu.make_async_remote_copy(
            src_ref=wsend.at[r // 2, side, c],
            dst_ref=wrecv.at[r // 2, 1 - side, c],
            send_sem=wss.at[r // 2, side, c],
            recv_sem=wrs.at[r // 2, 1 - side, c],
            device_id=(neighbour(i), v),
            device_id_type=MESH,
        )

    def before(r, c, i):
        wsend[r // 2, turn(i, 1), c] = inner(r, side_rows(i), x[c, side_rows(i)])

        @pl.when(reachable(i))
        def _():
            w_copy(r, c, i).start()

    ends = (slice(0, nb), slice(height - nb, height))

    def after(r, c):
        for i in (0, 1):
            @pl.when(reachable(i))
            def _():
                landed = wrecv.at[r // 2, turn(i, 1), c]
                pltpu.make_async_copy(landed, landed, wrs.at[r // 2, turn(i, 1), c]).wait()

        return [
            updated(r, rows, x[c, rows], wsend[r // 2, side, c] + wrecv[r // 2, side, c])
            for side, rows in enumerate(ends)
        ]

    def over_chunks(body):
        lax.fori_loop(0, chunks, lambda c, carry: (body(c), carry)[1], 0)

    for i in range(groups):
        g = turn(i, groups - 1)
        prepare_v(0, i)
        if i == 0:
            for entry in slots(1):
                send_t(1, *entry)
            send_round(2)
            send_round(3)
        arrived(0, g + 1, 0)
        form_u(0, g + 1, group_rows(i))
        if i == 0:
            for c in range(chunks):
                load(c).wait()
        over_chunks(lambda c: apply(0, c, group_rows(i)))
        if i == 0:
            prepare_v(1, 0)
            over_chunks(lambda c: before(1, c, 0))
            for r in range(4, rounds):
                send_round(r)
    prepare_v(1, 1)
    over_chunks(lambda c: before(1, c, 1))
    prepare_v(1, 2)
    prepare_u(1)
    for c in range(chunks):
        middle(1, c)

    for r in range(2, rounds, 2):
        prepare_v(r, 0)
        prepare_u(r)
        prepare_v(r + 1, 0)

        def step(c):
            head, tail = after(r - 1, c)
            whole = jnp.concatenate([head, x[c, nb : height - nb], tail], 0)
            spans = [slice(2 * nb * g, 2 * nb * (g + 1)) for g in range(groups)]
            shares = [inner(r, rows, whole[rows]) for rows in spans]
            values = [updated(r, rows, whole[rows], w) for rows, w in zip(spans, shares)]
            strips = (values[0][:nb], values[-1][nb:])
            shares = [inner(r + 1, rows, strip) for rows, strip in zip(ends, strips)]
            for side in (0, 1):
                wsend[(r + 1) // 2, side, c] = shares[side]
            for i in (0, 1):
                @pl.when(reachable(i))
                def _():
                    w_copy(r + 1, c, i).start()

            for rows, value in zip(spans, values):
                x[c, rows] = value

        over_chunks(step)
        prepare_u(r + 1)
        for c in range(chunks):
            middle(r + 1, c)

    def store(c):
        return pltpu.make_async_copy(
            x.at[c], out.at[:, pl.ds(pl.multiple_of(c * wide, wide), wide)], xout.at[c]
        )

    def finish(c):
        for rows, value in zip(ends, after(rounds - 1, c)):
            x[c, rows] = value
        store(c).start()

    over_chunks(finish)

    for r in range(rounds):
        for piece, where in enumerate(pieces(r)):
            for o in range(1, peers):
                v_copy(r, piece, where, o).wait_send()
        for slot, source, away in slots(r):
            for o in range(peers):
                if away == 0 and o != 0:
                    t_copy(r, slot, source, away, o).wait_send()
                elif away != 0:
                    @pl.when(d + away < count if o == 0 else d >= away)
                    def _():
                        t_copy(r, slot, source, away, o).wait_send()

    for i in (0, 1):
        @pl.when(reachable(i))
        def _():
            for r in range(1, rounds, 2):
                over_chunks(lambda c: w_copy(r, c, i).wait_send())

    over_chunks(lambda c: store(c).wait())


def solution(mesh):
    count, peers = mesh.shape["row"], mesh.shape["vec"]

    def per_device(eigvecs, reflectors, factors):
        height, width = eigvecs.shape
        rounds = reflectors.shape[0]
        nb = factors.shape[3]
        groups = height // (2 * nb)
        wide = width // CHUNKS
        f32, bf16, dma = jnp.float32, jnp.bfloat16, pltpu.SemaphoreType.DMA
        links = (rounds // 2, 2, CHUNKS)
        return pl.pallas_call(
            functools.partial(kernel, count, peers),
            out_shape=jax.ShapeDtypeStruct((height, width), f32),
            in_specs=[pl.BlockSpec(memory_space=pltpu.HBM)] * 3,
            out_specs=pl.BlockSpec(memory_space=pl.ANY),
            scratch_shapes=[
                pltpu.VMEM((CHUNKS, height, wide), f32),
                pltpu.VMEM((rounds, nb, height), f32),
                pltpu.VMEM((rounds, groups + 1, nb, nb), f32),
                pltpu.VMEM((rounds, 2 * nb, height), bf16),
                pltpu.VMEM((rounds, height, 3 * nb), bf16),
                pltpu.VMEM(links + (nb, wide), f32),
                pltpu.VMEM(links + (nb, wide), f32),
                dma((CHUNKS,)),
                dma((rounds, 3, peers)),
                dma((rounds, 3, peers)),
                dma((rounds, groups + 1, peers)),
                dma((rounds, groups + 1, peers)),
                dma(links),
                dma(links),
                dma((CHUNKS,)),
            ],
            compiler_params=pltpu.CompilerParams(
                collective_id=0, has_side_effects=True, vmem_limit_bytes=48 << 20
            ),
            name="back_transform",
        )(
            *(
                pltpu.with_memory_space_constraint(array, pltpu.HBM)
                for array in (eigvecs, jnp.transpose(reflectors, (0, 2, 1)), factors)
            )
        )

    return jax.shard_map(
        per_device,
        mesh=mesh,
        in_specs=(P("row", "vec"), P(None, "row", "vec"), P(None, "row", "vec", None)),
        out_specs=P("row", "vec"),
        check_vma=False,
    )
```

```python
import functools

import jax
import jax.numpy as jnp
from jax import lax
from jax.experimental import pallas as pl
from jax.experimental.pallas import tpu as pltpu
from jax.sharding import PartitionSpec as P

MESH = pl.DeviceIdType.MESH
CHUNKS = 4


def split(value):
    high = value.astype(jnp.bfloat16)
    return high, (value - high.astype(jnp.float32)).astype(jnp.bfloat16)


def dot(left, right):
    return lax.dot_general(
        left, right, (((1,), (0,)), ((), ())),
        precision=lax.Precision.DEFAULT, preferred_element_type=jnp.float32,
    )


def kernel(
    count, peers, eig, refl, fact, out,
    x, vt, tall, vcat, ucat, wsend, wrecv,
    xin, vsend, vrecv, tsend, trecv, hsend, hrecv, wss, wrs, xout,
):
    rounds, nb, height = vt.shape
    share = refl.shape[1]
    groups = height // (2 * nb)
    chunks, _, wide = x.shape
    d = lax.axis_index("row")
    v = lax.axis_index("vec")
    odd = lax.rem(d, 2)

    def peer(o):
        return lax.rem(v + o, peers)

    def rows_of(p):
        return pl.ds(pl.multiple_of(p * share, 8), share)

    def turn(i, last):
        return i + odd * (last - 2 * i)

    def group_rows(i):
        return pl.ds(pl.multiple_of(turn(i, groups - 1) * 2 * nb, nb), 2 * nb)

    def side_rows(i):
        return pl.ds(pl.multiple_of(turn(i, 1) * (height - nb), nb), nb)

    def middle_rows(g):
        return pl.ds(2 * nb * g + nb, 2 * nb)

    def pieces(r):
        if r == 0:
            return [group_rows(i) for i in range(groups)]
        if r % 2 == 1:
            return [side_rows(0), side_rows(1)] + [pl.ds(nb, height - 2 * nb)]
        return [pl.ds(0, height)]

    def slots(r):
        for k in range(-1 if r % 2 else 0, groups):
            q = k - r // 2
            yield k + 1, q % groups, -(q // groups)

    def sends_row(slot, away):
        there = d + away < count
        return jnp.logical_and(there, lax.rem(d + away, 2) == 0) if slot == 0 else there

    def takes_row(slot, away):
        return jnp.logical_and(d >= away, odd == 0) if slot == 0 else d >= away

    def head_copy(r):
        return pltpu.make_async_remote_copy(
            src_ref=tall.at[r, groups],
            dst_ref=tall.at[r, 0],
            send_sem=hsend.at[r],
            recv_sem=hrecv.at[r],
            device_id=(d + 1, v),
            device_id_type=MESH,
        )

    gives_head = jnp.logical_and(odd == 0, d + 1 < count)

    reach = max(away for r in range(rounds) for _, _, away in slots(r))

    def load(c):
        return pltpu.make_async_copy(eig.at[:, pl.ds(c * wide, wide)], x.at[c], xin.at[c])

    barrier = pltpu.get_barrier_semaphore()
    valid = jnp.int32(0)
    for away in range(-reach, reach + 1):
        inside = jnp.logical_and(d + away >= 0, d + away < count)
        valid = valid + inside.astype(jnp.int32)

        @pl.when(inside)
        def _():
            for o in range(peers):
                if away != 0 or o != 0:
                    pl.semaphore_signal(
                        barrier, inc=1, device_id=(d + away, peer(o)), device_id_type=MESH
                    )

    for c in range(chunks):
        load(c).start()
    pl.semaphore_wait(barrier, valid * peers - 1)

    def t_copy(r, slot, source, away, o):
        mine = tall.at[r, slot, rows_of(v)]
        return pltpu.make_async_remote_copy(
            src_ref=fact.at[r, source] if o == 0 or away == 0 else mine,
            dst_ref=mine,
            send_sem=tsend.at[r, slot, o],
            recv_sem=trecv.at[r, slot, o],
            device_id=(d + away if o == 0 else d, peer(o)),
            device_id_type=MESH,
        )

    def v_copy(r, piece, where, o):
        return pltpu.make_async_remote_copy(
            src_ref=refl.at[r, :, where],
            dst_ref=vt.at[r, rows_of(v), where],
            send_sem=vsend.at[r, piece, o],
            recv_sem=vrecv.at[r, piece, o],
            device_id=(d, peer(o)),
            device_id_type=MESH,
        )

    def send_v(r, piece):
        where = pieces(r)[piece]
        for o in range(1, peers):
            v_copy(r, piece, where, o).start()
        pltpu.make_async_copy(
            refl.at[r, :, where], vt.at[r, rows_of(v), where], vrecv.at[r, piece, 0]
        ).start()

    def own_t(r, slot, source):
        return pltpu.make_async_copy(
            fact.at[r, source], tall.at[r, slot, rows_of(v)], trecv.at[r, slot, 0]
        )

    def landed_t(r, slot, o):
        part = tall.at[r, slot, rows_of(lax.rem(v + peers - o, peers))]
        return pltpu.make_async_copy(part, part, trecv.at[r, slot, o])

    def send_t(r, slot, source, away):
        if away == 0:
            own_t(r, slot, source).start()
            for o in range(1, peers):
                t_copy(r, slot, source, away, o).start()
        else:
            @pl.when(takes_row(slot, away))
            def _():
                landed_t(r, slot, 0).wait()
                for o in range(1, peers):
                    t_copy(r, slot, source, away, o).start()

    def send_round(r):
        for piece in range(len(pieces(r))):
            send_v(r, piece)
        for entry in slots(r):
            send_t(r, *entry)

    send_v(0, 0)
    for r in range(rounds):
        for slot, source, away in slots(r):
            if away != 0:
                @pl.when(sends_row(slot, away))
                def _():
                    t_copy(r, slot, source, away, 0).start()
    for i in range(groups):
        g = turn(i, groups - 1)
        if i > 0:
            send_v(0, i)
        send_t(0, g + 1, g, 0)
        if i == 0:
            send_v(1, 0)
    send_v(1, 1)
    send_v(1, 2)

    @pl.when(d == 0)
    def _():
        wrecv[:, 0] = jnp.zeros((rounds // 2, chunks, nb, wide), jnp.float32)

    @pl.when(d == count - 1)
    def _():
        wrecv[:, 1] = jnp.zeros((rounds // 2, chunks, nb, wide), jnp.float32)

    def prepare_v(r, piece):
        where = pieces(r)[piece]
        for o in range(peers):
            part = vt.at[r, rows_of(lax.rem(v + peers - o, peers)), where]
            pltpu.make_async_copy(part, part, vrecv.at[r, piece, o]).wait()
        high, low = split(vt[r, :, where])
        vcat[r, :nb, where] = high
        vcat[r, nb:, where] = low

    def form_u(r, slot, where):
        bh, bl = split(jnp.transpose(vt[r, :, where]))
        th, tl = split(tall[r, slot])
        uh, ul = split(dot(bh, th) + dot(bh, tl) + dot(bl, th))
        ucat[r, where, :nb] = uh
        ucat[r, where, nb : 2 * nb] = ul
        ucat[r, where, 2 * nb :] = uh

    def arrived(r, slot, away):
        for o in range(0 if away == 0 else 1, peers):
            landed_t(r, slot, o).wait()

    def prepare_u(r):
        for slot, _, away in reversed(list(slots(r))):
            if away == 0:
                arrived(r, slot, away)
            else:
                @pl.when(takes_row(slot, away))
                def _():
                    arrived(r, slot, away)

                @pl.when(d < away if slot else jnp.logical_and(d < away, odd == 0))
                def _():
                    tall[r, slot] = jnp.zeros((nb, nb), jnp.float32)

            if r % 2 == 1 and slot == groups:
                @pl.when(gives_head)
                def _():
                    head_copy(r).start()

            if slot == 0:
                @pl.when(odd == 1)
                def _():
                    head_copy(r).wait_recv()

            first = (slot - 1) * 2 * nb + (r % 2) * nb
            begin, end = max(first, 0), min(first + 2 * nb, height)
            form_u(r, slot, pl.ds(begin, end - begin))

    def inner(r, rows, value):
        xh, xl = split(value)
        both = dot(vcat[r, :, rows], xh)
        return both[:nb] + both[nb:] + dot(vcat[r, :nb, rows], xl)

    def updated(r, rows, value, w):
        wh, wl = split(w)
        stacked = jnp.concatenate([wh, wh, wl], 0)
        return value - dot(ucat[r, rows], stacked)

    def apply(r, c, rows):
        value = x[c, rows]
        x[c, rows] = updated(r, rows, value, inner(r, rows, value))

    def middle(r, c):
        for g in range(groups - 1):
            apply(r, c, middle_rows(g))

    def neighbour(i):
        return d + 2 * turn(i, 1) - 1

    def reachable(i):
        return jnp.logical_and(neighbour(i) >= 0, neighbour(i) < count)

    def w_copy(r, c, i):
        side = turn(i, 1)
        return pltpu.make_async_remote_copy(
            src_ref=wsend.at[r // 2, side, c],
            dst_ref=wrecv.at[r // 2, 1 - side, c],
            send_sem=wss.at[r // 2, side, c],
            recv_sem=wrs.at[r // 2, 1 - side, c],
            device_id=(neighbour(i), v),
            device_id_type=MESH,
        )

    def first(c, i, side):
        rows = group_rows(i)
        value = x[c, rows]
        value = updated(0, rows, value, inner(0, rows, value))
        if side is not None:
            strip = jnp.where(odd == side, value[:nb], value[nb:])
            wsend[0, turn(side, 1), c] = inner(1, side_rows(side), strip)

            @pl.when(reachable(side))
            def _():
                w_copy(1, c, side).start()

        x[c, rows] = value

    ends = (slice(0, nb), slice(height - nb, height))

    def after(r, c):
        for i in (0, 1):
            @pl.when(reachable(i))
            def _():
                landed = wrecv.at[r // 2, turn(i, 1), c]
                pltpu.make_async_copy(landed, landed, wrs.at[r // 2, turn(i, 1), c]).wait()

        return [
            updated(r, rows, x[c, rows], wsend[r // 2, side, c] + wrecv[r // 2, side, c])
            for side, rows in enumerate(ends)
        ]

    def over_chunks(body):
        lax.fori_loop(0, chunks, lambda c, carry: (body(c), carry)[1], 0)

    for i in range(groups):
        g = turn(i, groups - 1)
        prepare_v(0, i)
        if i == 0:
            for entry in slots(1):
                send_t(1, *entry)
            send_round(2)
            send_round(3)
        arrived(0, g + 1, 0)
        form_u(0, g + 1, group_rows(i))
        if i == 0:
            for c in range(chunks):
                load(c).wait()
        side = {0: 0, groups - 1: 1}.get(i)
        if side is not None:
            prepare_v(1, side)
        over_chunks(lambda c: first(c, i, side))
        if i == 0:
            for r in range(4, rounds):
                send_round(r)
    prepare_v(1, 2)
    prepare_u(1)
    for c in range(chunks):
        middle(1, c)

    for r in range(2, rounds, 2):
        prepare_v(r, 0)
        prepare_u(r)
        prepare_v(r + 1, 0)
        prepare_v(r + 1, 1)

        def step(c):
            head, tail = after(r - 1, c)
            whole = jnp.concatenate([head, x[c, nb : height - nb], tail], 0)
            spans = [slice(2 * nb * g, 2 * nb * (g + 1)) for g in range(groups)]
            shares = [inner(r, rows, whole[rows]) for rows in spans]
            values = [updated(r, rows, whole[rows], w) for rows, w in zip(spans, shares)]
            strips = (values[0][:nb], values[-1][nb:])
            shares = [inner(r + 1, rows, strip) for rows, strip in zip(ends, strips)]
            for side in (0, 1):
                wsend[(r + 1) // 2, side, c] = shares[side]
            for i in (0, 1):
                @pl.when(reachable(i))
                def _():
                    w_copy(r + 1, c, i).start()

            for rows, value in zip(spans, values):
                x[c, rows] = value

        over_chunks(step)
        prepare_v(r + 1, 2)
        prepare_u(r + 1)
        for c in range(chunks):
            middle(r + 1, c)

    def store(c):
        return pltpu.make_async_copy(
            x.at[c], out.at[:, pl.ds(pl.multiple_of(c * wide, wide), wide)], xout.at[c]
        )

    def finish(c):
        for rows, value in zip(ends, after(rounds - 1, c)):
            x[c, rows] = value
        store(c).start()

    over_chunks(finish)

    for r in range(rounds):
        for piece, where in enumerate(pieces(r)):
            for o in range(1, peers):
                v_copy(r, piece, where, o).wait_send()
        for slot, source, away in slots(r):
            for o in range(peers):
                if away == 0 and o != 0:
                    t_copy(r, slot, source, away, o).wait_send()
                elif away != 0:
                    @pl.when(sends_row(slot, away) if o == 0 else takes_row(slot, away))
                    def _():
                        t_copy(r, slot, source, away, o).wait_send()

    for i in (0, 1):
        @pl.when(reachable(i))
        def _():
            for r in range(1, rounds, 2):
                over_chunks(lambda c: w_copy(r, c, i).wait_send())

    @pl.when(gives_head)
    def _():
        for r in range(1, rounds, 2):
            head_copy(r).wait_send()

    over_chunks(lambda c: store(c).wait())


def solution(mesh):
    count, peers = mesh.shape["row"], mesh.shape["vec"]

    def per_device(eigvecs, reflectors, factors):
        height, width = eigvecs.shape
        rounds = reflectors.shape[0]
        nb = factors.shape[3]
        groups = height // (2 * nb)
        wide = width // CHUNKS
        f32, bf16, dma = jnp.float32, jnp.bfloat16, pltpu.SemaphoreType.DMA
        links = (rounds // 2, 2, CHUNKS)
        return pl.pallas_call(
            functools.partial(kernel, count, peers),
            out_shape=jax.ShapeDtypeStruct((height, width), f32),
            in_specs=[pl.BlockSpec(memory_space=pltpu.HBM)] * 3,
            out_specs=pl.BlockSpec(memory_space=pl.ANY),
            scratch_shapes=[
                pltpu.VMEM((CHUNKS, height, wide), f32),
                pltpu.VMEM((rounds, nb, height), f32),
                pltpu.VMEM((rounds, groups + 1, nb, nb), f32),
                pltpu.VMEM((rounds, 2 * nb, height), bf16),
                pltpu.VMEM((rounds, height, 3 * nb), bf16),
                pltpu.VMEM(links + (nb, wide), f32),
                pltpu.VMEM(links + (nb, wide), f32),
                dma((CHUNKS,)),
                dma((rounds, 3, peers)),
                dma((rounds, 3, peers)),
                dma((rounds, groups + 1, peers)),
                dma((rounds, groups + 1, peers)),
                dma((rounds,)),
                dma((rounds,)),
                dma(links),
                dma(links),
                dma((CHUNKS,)),
            ],
            compiler_params=pltpu.CompilerParams(
                collective_id=0, has_side_effects=True, vmem_limit_bytes=48 << 20
            ),
            name="back_transform",
        )(
            *(
                pltpu.with_memory_space_constraint(array, pltpu.HBM)
                for array in (eigvecs, jnp.transpose(reflectors, (0, 2, 1)), factors)
            )
        )

    return jax.shard_map(
        per_device,
        mesh=mesh,
        in_specs=(P("row", "vec"), P(None, "row", "vec"), P(None, "row", "vec", None)),
        out_specs=P("row", "vec"),
        check_vma=False,
    )
```

```python
import functools

import jax
import jax.numpy as jnp
from jax import lax
from jax.experimental import pallas as pl
from jax.experimental.pallas import tpu as pltpu
from jax.sharding import PartitionSpec as P

MESH = pl.DeviceIdType.MESH
CHUNKS = 4


def split(value):
    high = value.astype(jnp.bfloat16)
    return high, (value - high.astype(jnp.float32)).astype(jnp.bfloat16)


def dot(left, right):
    return lax.dot_general(
        left, right, (((1,), (0,)), ((), ())),
        precision=lax.Precision.DEFAULT, preferred_element_type=jnp.float32,
    )


def kernel(
    count, peers, eig, refl, fact, out,
    x, vt, tall, vcat, ucat, wsend, wrecv,
    xin, vsend, vrecv, tsend, trecv, hsend, hrecv, wss, wrs, xout,
):
    rounds, nb, height = vt.shape
    share = refl.shape[1]
    groups = height // (2 * nb)
    chunks, _, wide = x.shape
    d = lax.axis_index("row")
    v = lax.axis_index("vec")
    odd = lax.rem(d, 2)

    def peer(o):
        return lax.rem(v + o, peers)

    def rows_of(p):
        return pl.ds(pl.multiple_of(p * share, 8), share)

    def turn(i, last):
        return i + odd * (last - 2 * i)

    def group_rows(i):
        return pl.ds(pl.multiple_of(turn(i, groups - 1) * 2 * nb, nb), 2 * nb)

    def side_rows(i):
        return pl.ds(pl.multiple_of(turn(i, 1) * (height - nb), nb), nb)

    def middle_rows(g):
        return pl.ds(2 * nb * g + nb, 2 * nb)

    def pieces(r):
        if r == 0:
            return [group_rows(i) for i in range(groups)]
        if r % 2 == 1:
            return [side_rows(0), side_rows(1)] + [pl.ds(nb, height - 2 * nb)]
        return [pl.ds(0, height)]

    def slots(r):
        for k in range(-1 if r % 2 else 0, groups):
            q = k - r // 2
            yield k + 1, q % groups, -(q // groups)

    def sends_row(slot, away):
        there = d + away < count
        return jnp.logical_and(there, lax.rem(d + away, 2) == 0) if slot == 0 else there

    def takes_row(slot, away):
        return jnp.logical_and(d >= away, odd == 0) if slot == 0 else d >= away

    def head_copy(r):
        return pltpu.make_async_remote_copy(
            src_ref=tall.at[r, groups],
            dst_ref=tall.at[r, 0],
            send_sem=hsend.at[r],
            recv_sem=hrecv.at[r],
            device_id=(d + 1, v),
            device_id_type=MESH,
        )

    gives_head = jnp.logical_and(odd == 0, d + 1 < count)

    reach = max(away for r in range(rounds) for _, _, away in slots(r))

    def load(c):
        return pltpu.make_async_copy(eig.at[:, pl.ds(c * wide, wide)], x.at[c], xin.at[c])

    barrier = pltpu.get_barrier_semaphore()
    valid = jnp.int32(0)
    for away in range(-reach, reach + 1):
        inside = jnp.logical_and(d + away >= 0, d + away < count)
        partners = [o for o in range(peers) if (away == 0) != (o == 0)]
        valid = valid + inside.astype(jnp.int32) * len(partners)

        @pl.when(inside)
        def _():
            for o in partners:
                pl.semaphore_signal(
                    barrier, inc=1, device_id=(d + away, peer(o)), device_id_type=MESH
                )

    for c in range(chunks):
        load(c).start()
    pl.semaphore_wait(barrier, valid)

    def t_copy(r, slot, source, away, o):
        mine = tall.at[r, slot, rows_of(v)]
        return pltpu.make_async_remote_copy(
            src_ref=fact.at[r, source] if o == 0 or away == 0 else mine,
            dst_ref=mine,
            send_sem=tsend.at[r, slot, o],
            recv_sem=trecv.at[r, slot, o],
            device_id=(d + away if o == 0 else d, peer(o)),
            device_id_type=MESH,
        )

    def v_copy(r, piece, where, o):
        return pltpu.make_async_remote_copy(
            src_ref=refl.at[r, :, where],
            dst_ref=vt.at[r, rows_of(v), where],
            send_sem=vsend.at[r, piece, o],
            recv_sem=vrecv.at[r, piece, o],
            device_id=(d, peer(o)),
            device_id_type=MESH,
        )

    def send_v(r, piece):
        where = pieces(r)[piece]
        for o in range(1, peers):
            v_copy(r, piece, where, o).start()
        pltpu.make_async_copy(
            refl.at[r, :, where], vt.at[r, rows_of(v), where], vrecv.at[r, piece, 0]
        ).start()

    def own_t(r, slot, source):
        return pltpu.make_async_copy(
            fact.at[r, source], tall.at[r, slot, rows_of(v)], trecv.at[r, slot, 0]
        )

    def landed_t(r, slot, o):
        part = tall.at[r, slot, rows_of(lax.rem(v + peers - o, peers))]
        return pltpu.make_async_copy(part, part, trecv.at[r, slot, o])

    def send_t(r, slot, source, away):
        if away == 0:
            own_t(r, slot, source).start()
            for o in range(1, peers):
                t_copy(r, slot, source, away, o).start()
        else:
            @pl.when(takes_row(slot, away))
            def _():
                landed_t(r, slot, 0).wait()
                for o in range(1, peers):
                    t_copy(r, slot, source, away, o).start()

    def send_round(r):
        for piece in range(len(pieces(r))):
            send_v(r, piece)
        for entry in slots(r):
            send_t(r, *entry)

    send_v(0, 0)
    for r in range(rounds):
        for slot, source, away in slots(r):
            if away != 0:
                @pl.when(sends_row(slot, away))
                def _():
                    t_copy(r, slot, source, away, 0).start()
    for i in range(groups):
        g = turn(i, groups - 1)
        if i > 0:
            send_v(0, i)
        send_t(0, g + 1, g, 0)
        if i == 0:
            send_v(1, 0)
    send_v(1, 1)
    send_v(1, 2)

    @pl.when(d == 0)
    def _():
        wrecv[:, 0] = jnp.zeros((rounds // 2, chunks, nb, wide), jnp.float32)

    @pl.when(d == count - 1)
    def _():
        wrecv[:, 1] = jnp.zeros((rounds // 2, chunks, nb, wide), jnp.float32)

    def prepare_v(r, piece):
        where = pieces(r)[piece]
        for o in range(peers):
            part = vt.at[r, rows_of(lax.rem(v + peers - o, peers)), where]
            pltpu.make_async_copy(part, part, vrecv.at[r, piece, o]).wait()
        high, low = split(vt[r, :, where])
        vcat[r, :nb, where] = high
        vcat[r, nb:, where] = low

    def form_u(r, slot, where):
        bh, bl = split(jnp.transpose(vt[r, :, where]))
        th, tl = split(tall[r, slot])
        uh, ul = split(dot(bh, th) + dot(bh, tl) + dot(bl, th))
        ucat[r, where, :nb] = uh
        ucat[r, where, nb : 2 * nb] = ul
        ucat[r, where, 2 * nb :] = uh

    def arrived(r, slot, away):
        for o in range(0 if away == 0 else 1, peers):
            landed_t(r, slot, o).wait()

    def prepare_u(r):
        for slot, _, away in reversed(list(slots(r))):
            if away == 0:
                arrived(r, slot, away)
            else:
                @pl.when(takes_row(slot, away))
                def _():
                    arrived(r, slot, away)

                @pl.when(d < away if slot else jnp.logical_and(d < away, odd == 0))
                def _():
                    tall[r, slot] = jnp.zeros((nb, nb), jnp.float32)

            if r % 2 == 1 and slot == groups:
                @pl.when(gives_head)
                def _():
                    head_copy(r).start()

            if slot == 0:
                @pl.when(odd == 1)
                def _():
                    head_copy(r).wait_recv()

            first = (slot - 1) * 2 * nb + (r % 2) * nb
            begin, end = max(first, 0), min(first + 2 * nb, height)
            form_u(r, slot, pl.ds(begin, end - begin))

    def inner(r, rows, value):
        xh, xl = split(value)
        both = dot(vcat[r, :, rows], xh)
        return both[:nb] + both[nb:] + dot(vcat[r, :nb, rows], xl)

    def updated(r, rows, value, w):
        wh, wl = split(w)
        stacked = jnp.concatenate([wh, wh, wl], 0)
        return value - dot(ucat[r, rows], stacked)

    def apply(r, c, rows):
        value = x[c, rows]
        x[c, rows] = updated(r, rows, value, inner(r, rows, value))

    def middle(r, c):
        for g in range(groups - 1):
            apply(r, c, middle_rows(g))

    def neighbour(i):
        return d + 2 * turn(i, 1) - 1

    def reachable(i):
        return jnp.logical_and(neighbour(i) >= 0, neighbour(i) < count)

    def w_copy(r, c, i):
        side = turn(i, 1)
        return pltpu.make_async_remote_copy(
            src_ref=wsend.at[r // 2, side, c],
            dst_ref=wrecv.at[r // 2, 1 - side, c],
            send_sem=wss.at[r // 2, side, c],
            recv_sem=wrs.at[r // 2, 1 - side, c],
            device_id=(neighbour(i), v),
            device_id_type=MESH,
        )

    def first(c, i, side):
        rows = group_rows(i)
        value = x[c, rows]
        value = updated(0, rows, value, inner(0, rows, value))
        if side is not None:
            strip = jnp.where(odd == side, value[:nb], value[nb:])
            wsend[0, turn(side, 1), c] = inner(1, side_rows(side), strip)

            @pl.when(reachable(side))
            def _():
                w_copy(1, c, side).start()

        x[c, rows] = value

    ends = (slice(0, nb), slice(height - nb, height))

    def after(r, c):
        for i in (0, 1):
            @pl.when(reachable(i))
            def _():
                landed = wrecv.at[r // 2, turn(i, 1), c]
                pltpu.make_async_copy(landed, landed, wrs.at[r // 2, turn(i, 1), c]).wait()

        return [
            updated(r, rows, x[c, rows], wsend[r // 2, side, c] + wrecv[r // 2, side, c])
            for side, rows in enumerate(ends)
        ]

    def over_chunks(body):
        lax.fori_loop(0, chunks, lambda c, carry: (body(c), carry)[1], 0)

    for i in range(groups):
        g = turn(i, groups - 1)
        prepare_v(0, i)
        arrived(0, g + 1, 0)
        form_u(0, g + 1, group_rows(i))
        if i == 0:
            for c in range(chunks):
                load(c).wait()
        side = {0: 0, groups - 1: 1}.get(i)
        if side is not None:
            prepare_v(1, side)
        over_chunks(lambda c: first(c, i, side))
        if i == 0:
            for entry in slots(1):
                send_t(1, *entry)
            send_round(2)
            send_round(3)
        if i == groups - 1:
            for r in range(4, rounds):
                send_round(r)
    prepare_v(1, 2)
    prepare_u(1)
    for c in range(chunks):
        middle(1, c)

    for r in range(2, rounds, 2):
        prepare_v(r, 0)
        prepare_u(r)
        prepare_v(r + 1, 0)
        prepare_v(r + 1, 1)

        def step(c):
            head, tail = after(r - 1, c)
            whole = jnp.concatenate([head, x[c, nb : height - nb], tail], 0)
            spans = [slice(2 * nb * g, 2 * nb * (g + 1)) for g in range(groups)]
            shares = [inner(r, rows, whole[rows]) for rows in spans]
            values = [updated(r, rows, whole[rows], w) for rows, w in zip(spans, shares)]
            strips = (values[0][:nb], values[-1][nb:])
            shares = [inner(r + 1, rows, strip) for rows, strip in zip(ends, strips)]
            for side in (0, 1):
                wsend[(r + 1) // 2, side, c] = shares[side]
            for i in (0, 1):
                @pl.when(reachable(i))
                def _():
                    w_copy(r + 1, c, i).start()

            for rows, value in zip(spans, values):
                x[c, rows] = value

        over_chunks(step)
        prepare_v(r + 1, 2)
        prepare_u(r + 1)
        for c in range(chunks):
            middle(r + 1, c)

    def store(c):
        return pltpu.make_async_copy(
            x.at[c], out.at[:, pl.ds(pl.multiple_of(c * wide, wide), wide)], xout.at[c]
        )

    def finish(c):
        for rows, value in zip(ends, after(rounds - 1, c)):
            x[c, rows] = value
        store(c).start()

    over_chunks(finish)

    for r in range(rounds):
        for piece, where in enumerate(pieces(r)):
            for o in range(1, peers):
                v_copy(r, piece, where, o).wait_send()
        for slot, source, away in slots(r):
            for o in range(peers):
                if away == 0 and o != 0:
                    t_copy(r, slot, source, away, o).wait_send()
                elif away != 0:
                    @pl.when(sends_row(slot, away) if o == 0 else takes_row(slot, away))
                    def _():
                        t_copy(r, slot, source, away, o).wait_send()

    for i in (0, 1):
        @pl.when(reachable(i))
        def _():
            for r in range(1, rounds, 2):
                over_chunks(lambda c: w_copy(r, c, i).wait_send())

    @pl.when(gives_head)
    def _():
        for r in range(1, rounds, 2):
            head_copy(r).wait_send()

    over_chunks(lambda c: store(c).wait())


def solution(mesh):
    count, peers = mesh.shape["row"], mesh.shape["vec"]

    def per_device(eigvecs, reflectors, factors):
        height, width = eigvecs.shape
        rounds = reflectors.shape[0]
        nb = factors.shape[3]
        groups = height // (2 * nb)
        wide = width // CHUNKS
        f32, bf16, dma = jnp.float32, jnp.bfloat16, pltpu.SemaphoreType.DMA
        links = (rounds // 2, 2, CHUNKS)
        return pl.pallas_call(
            functools.partial(kernel, count, peers),
            out_shape=jax.ShapeDtypeStruct((height, width), f32),
            in_specs=[pl.BlockSpec(memory_space=pltpu.HBM)] * 3,
            out_specs=pl.BlockSpec(memory_space=pl.ANY),
            scratch_shapes=[
                pltpu.VMEM((CHUNKS, height, wide), f32),
                pltpu.VMEM((rounds, nb, height), f32),
                pltpu.VMEM((rounds, groups + 1, nb, nb), f32),
                pltpu.VMEM((rounds, 2 * nb, height), bf16),
                pltpu.VMEM((rounds, height, 3 * nb), bf16),
                pltpu.VMEM(links + (nb, wide), f32),
                pltpu.VMEM(links + (nb, wide), f32),
                dma((CHUNKS,)),
                dma((rounds, 3, peers)),
                dma((rounds, 3, peers)),
                dma((rounds, groups + 1, peers)),
                dma((rounds, groups + 1, peers)),
                dma((rounds,)),
                dma((rounds,)),
                dma(links),
                dma(links),
                dma((CHUNKS,)),
            ],
            compiler_params=pltpu.CompilerParams(
                collective_id=0, has_side_effects=True, vmem_limit_bytes=48 << 20
            ),
            name="back_transform",
        )(
            *(
                pltpu.with_memory_space_constraint(array, pltpu.HBM)
                for array in (eigvecs, jnp.transpose(reflectors, (0, 2, 1)), factors)
            )
        )

    return jax.shard_map(
        per_device,
        mesh=mesh,
        in_specs=(P("row", "vec"), P(None, "row", "vec"), P(None, "row", "vec", None)),
        out_specs=P("row", "vec"),
        check_vma=False,
    )
```

```python
import functools

import jax
import jax.numpy as jnp
from jax import lax
from jax.experimental import pallas as pl
from jax.experimental.pallas import tpu as pltpu
from jax.sharding import PartitionSpec as P

MESH = pl.DeviceIdType.MESH
CHUNKS = 4


def split(value):
    high = value.astype(jnp.bfloat16)
    return high, (value - high.astype(jnp.float32)).astype(jnp.bfloat16)


def dot(left, right):
    return lax.dot_general(
        left, right, (((1,), (0,)), ((), ())),
        precision=lax.Precision.DEFAULT, preferred_element_type=jnp.float32,
    )


def kernel(
    count, peers, eig, refl, fact, out,
    x, vt, tall, vcat, ucat, wsend, wrecv,
    xin, vsend, vrecv, tsend, trecv, hsend, hrecv, wss, wrs, xout,
):
    rounds, nb, height = vt.shape
    share = refl.shape[1]
    groups = height // (2 * nb)
    chunks, _, wide = x.shape
    d = lax.axis_index("row")
    v = lax.axis_index("vec")
    odd = lax.rem(d, 2)

    def peer(o):
        return lax.rem(v + o, peers)

    def rows_of(p):
        return pl.ds(pl.multiple_of(p * share, 8), share)

    def turn(i, last):
        return i + odd * (last - 2 * i)

    def group_rows(i):
        return pl.ds(pl.multiple_of(turn(i, groups - 1) * 2 * nb, nb), 2 * nb)

    def side_rows(i):
        return pl.ds(pl.multiple_of(turn(i, 1) * (height - nb), nb), nb)

    def middle_rows(g):
        return pl.ds(2 * nb * g + nb, 2 * nb)

    def pieces(r):
        if r == 0:
            return [group_rows(i) for i in range(groups)]
        if r % 2 == 1:
            return [side_rows(0), side_rows(1)] + [pl.ds(nb, height - 2 * nb)]
        return [pl.ds(0, height)]

    def slots(r):
        for k in range(-1 if r % 2 else 0, groups):
            q = k - r // 2
            yield k + 1, q % groups, -(q // groups)

    def sends_row(slot, away):
        there = d + away < count
        return jnp.logical_and(there, lax.rem(d + away, 2) == 0) if slot == 0 else there

    def takes_row(slot, away):
        return jnp.logical_and(d >= away, odd == 0) if slot == 0 else d >= away

    def head_copy(r):
        return pltpu.make_async_remote_copy(
            src_ref=tall.at[r, groups],
            dst_ref=tall.at[r, 0],
            send_sem=hsend.at[r],
            recv_sem=hrecv.at[r],
            device_id=(d + 1, v),
            device_id_type=MESH,
        )

    gives_head = jnp.logical_and(odd == 0, d + 1 < count)

    reach = max(away for r in range(rounds) for _, _, away in slots(r))

    def load(c):
        return pltpu.make_async_copy(eig.at[:, pl.ds(c * wide, wide)], x.at[c], xin.at[c])

    barrier = pltpu.get_barrier_semaphore()
    valid = jnp.int32(0)
    for away in range(-reach, reach + 1):
        inside = jnp.logical_and(d + away >= 0, d + away < count)
        partners = [o for o in range(peers) if (away == 0) != (o == 0)]
        valid = valid + inside.astype(jnp.int32) * len(partners)

        @pl.when(inside)
        def _():
            for o in partners:
                pl.semaphore_signal(
                    barrier, inc=1, device_id=(d + away, peer(o)), device_id_type=MESH
                )

    for c in range(chunks):
        load(c).start()
    pl.semaphore_wait(barrier, valid)

    def t_copy(r, slot, source, away, o):
        mine = tall.at[r, slot, rows_of(v)]
        return pltpu.make_async_remote_copy(
            src_ref=fact.at[r, source] if o == 0 or away == 0 else mine,
            dst_ref=mine,
            send_sem=tsend.at[r, slot, o],
            recv_sem=trecv.at[r, slot, o],
            device_id=(d + away if o == 0 else d, peer(o)),
            device_id_type=MESH,
        )

    def v_copy(r, piece, where, o):
        return pltpu.make_async_remote_copy(
            src_ref=refl.at[r, :, where],
            dst_ref=vt.at[r, rows_of(v), where],
            send_sem=vsend.at[r, piece, o],
            recv_sem=vrecv.at[r, piece, o],
            device_id=(d, peer(o)),
            device_id_type=MESH,
        )

    def send_v(r, piece):
        where = pieces(r)[piece]
        for o in range(1, peers):
            v_copy(r, piece, where, o).start()
        pltpu.make_async_copy(
            refl.at[r, :, where], vt.at[r, rows_of(v), where], vrecv.at[r, piece, 0]
        ).start()

    def own_t(r, slot, source):
        return pltpu.make_async_copy(
            fact.at[r, source], tall.at[r, slot, rows_of(v)], trecv.at[r, slot, 0]
        )

    def landed_t(r, slot, o):
        part = tall.at[r, slot, rows_of(lax.rem(v + peers - o, peers))]
        return pltpu.make_async_copy(part, part, trecv.at[r, slot, o])

    def send_t(r, slot, source, away):
        if away == 0:
            own_t(r, slot, source).start()
            for o in range(1, peers):
                t_copy(r, slot, source, away, o).start()
        else:
            @pl.when(takes_row(slot, away))
            def _():
                landed_t(r, slot, 0).wait()
                for o in range(1, peers):
                    t_copy(r, slot, source, away, o).start()

    def send_round(r):
        for piece in range(len(pieces(r))):
            send_v(r, piece)
        for entry in slots(r):
            send_t(r, *entry)

    send_v(0, 0)
    for r in range(rounds):
        for slot, source, away in slots(r):
            if away != 0:
                @pl.when(sends_row(slot, away))
                def _():
                    t_copy(r, slot, source, away, 0).start()
    for i in range(groups):
        g = turn(i, groups - 1)
        if i > 0:
            send_v(0, i)
        send_t(0, g + 1, g, 0)
        if i == 0:
            send_v(1, 0)
    send_v(1, 1)
    send_v(1, 2)

    @pl.when(d == 0)
    def _():
        wrecv[:, 0] = jnp.zeros((rounds // 2, chunks, nb, wide), jnp.float32)

    @pl.when(d == count - 1)
    def _():
        wrecv[:, 1] = jnp.zeros((rounds // 2, chunks, nb, wide), jnp.float32)

    def prepare_v(r, piece):
        where = pieces(r)[piece]
        for o in range(peers):
            part = vt.at[r, rows_of(lax.rem(v + peers - o, peers)), where]
            pltpu.make_async_copy(part, part, vrecv.at[r, piece, o]).wait()
        high, low = split(vt[r, :, where])
        vcat[r, :nb, where] = high
        vcat[r, nb:, where] = low

    def form_u(r, slot, where):
        bh, bl = split(jnp.transpose(vt[r, :, where]))
        th, tl = split(tall[r, slot])
        uh, ul = split(dot(bh, th) + dot(bh, tl) + dot(bl, th))
        ucat[r, where, :nb] = uh
        ucat[r, where, nb : 2 * nb] = ul
        ucat[r, where, 2 * nb :] = uh

    def arrived(r, slot, away):
        for o in range(0 if away == 0 else 1, peers):
            landed_t(r, slot, o).wait()

    def prepare_u(r):
        for slot, _, away in reversed(list(slots(r))):
            if away == 0:
                arrived(r, slot, away)
            else:
                @pl.when(takes_row(slot, away))
                def _():
                    arrived(r, slot, away)

                @pl.when(d < away if slot else jnp.logical_and(d < away, odd == 0))
                def _():
                    tall[r, slot] = jnp.zeros((nb, nb), jnp.float32)

            if r % 2 == 1 and slot == groups:
                @pl.when(gives_head)
                def _():
                    head_copy(r).start()

            if slot == 0:
                @pl.when(odd == 1)
                def _():
                    head_copy(r).wait_recv()

            first = (slot - 1) * 2 * nb + (r % 2) * nb
            begin, end = max(first, 0), min(first + 2 * nb, height)
            form_u(r, slot, pl.ds(begin, end - begin))

    def inner(r, rows, value):
        xh, xl = split(value)
        both = dot(vcat[r, :, rows], xh)
        return both[:nb] + both[nb:] + dot(vcat[r, :nb, rows], xl)

    def updated(r, rows, value, w):
        wh, wl = split(w)
        stacked = jnp.concatenate([wh, wh, wl], 0)
        return value - dot(ucat[r, rows], stacked)

    def apply(r, c, rows):
        value = x[c, rows]
        x[c, rows] = updated(r, rows, value, inner(r, rows, value))

    def middle(r, c):
        for g in range(groups - 1):
            apply(r, c, middle_rows(g))

    def neighbour(i):
        return d + 2 * turn(i, 1) - 1

    def reachable(i):
        return jnp.logical_and(neighbour(i) >= 0, neighbour(i) < count)

    def w_copy(r, c, i):
        side = turn(i, 1)
        return pltpu.make_async_remote_copy(
            src_ref=wsend.at[r // 2, side, c],
            dst_ref=wrecv.at[r // 2, 1 - side, c],
            send_sem=wss.at[r // 2, side, c],
            recv_sem=wrs.at[r // 2, 1 - side, c],
            device_id=(neighbour(i), v),
            device_id_type=MESH,
        )

    def first(c, i, side):
        rows = group_rows(i)
        value = x[c, rows]
        value = updated(0, rows, value, inner(0, rows, value))
        if side is not None:
            strip = jnp.where(odd == side, value[:nb], value[nb:])
            wsend[0, turn(side, 1), c] = inner(1, side_rows(side), strip)

            @pl.when(reachable(side))
            def _():
                w_copy(1, c, side).start()

        x[c, rows] = value

    ends = (slice(0, nb), slice(height - nb, height))

    def after(r, c):
        for i in (0, 1):
            @pl.when(reachable(i))
            def _():
                landed = wrecv.at[r // 2, turn(i, 1), c]
                pltpu.make_async_copy(landed, landed, wrs.at[r // 2, turn(i, 1), c]).wait()

        return [
            updated(r, rows, x[c, rows], wsend[r // 2, side, c] + wrecv[r // 2, side, c])
            for side, rows in enumerate(ends)
        ]

    def over_chunks(body):
        lax.fori_loop(0, chunks, lambda c, carry: (body(c), carry)[1], 0)

    for i in range(groups):
        g = turn(i, groups - 1)
        prepare_v(0, i)
        if i == 0:
            for entry in slots(1):
                send_t(1, *entry)
            send_round(2)
            send_round(3)
        arrived(0, g + 1, 0)
        form_u(0, g + 1, group_rows(i))
        if i == 0:
            for c in range(chunks):
                load(c).wait()
        side = {0: 0, groups - 1: 1}.get(i)
        if side is not None:
            prepare_v(1, side)
        over_chunks(lambda c: first(c, i, side))
        if i == 0:
            for r in range(4, rounds):
                send_round(r)
    prepare_v(1, 2)
    prepare_u(1)
    for c in range(chunks):
        middle(1, c)

    for r in range(2, rounds, 2):
        prepare_v(r, 0)
        prepare_u(r)
        prepare_v(r + 1, 0)
        prepare_v(r + 1, 1)

        def step(c):
            head, tail = after(r - 1, c)
            whole = jnp.concatenate([head, x[c, nb : height - nb], tail], 0)
            spans = [slice(2 * nb * g, 2 * nb * (g + 1)) for g in range(groups)]
            shares = [inner(r, rows, whole[rows]) for rows in spans]
            values = [updated(r, rows, whole[rows], w) for rows, w in zip(spans, shares)]
            strips = (values[0][:nb], values[-1][nb:])
            shares = [inner(r + 1, rows, strip) for rows, strip in zip(ends, strips)]
            for side in (0, 1):
                wsend[(r + 1) // 2, side, c] = shares[side]
            for i in (0, 1):
                @pl.when(reachable(i))
                def _():
                    w_copy(r + 1, c, i).start()

            for rows, value in zip(spans, values):
                x[c, rows] = value

        over_chunks(step)
        prepare_v(r + 1, 2)
        prepare_u(r + 1)
        for c in range(chunks):
            middle(r + 1, c)

    def store(c):
        return pltpu.make_async_copy(
            x.at[c], out.at[:, pl.ds(pl.multiple_of(c * wide, wide), wide)], xout.at[c]
        )

    def finish(c):
        for rows, value in zip(ends, after(rounds - 1, c)):
            x[c, rows] = value
        store(c).start()

    over_chunks(finish)

    for r in range(rounds):
        for piece, where in enumerate(pieces(r)):
            for o in range(1, peers):
                v_copy(r, piece, where, o).wait_send()
        for slot, source, away in slots(r):
            for o in range(peers):
                if away == 0 and o != 0:
                    t_copy(r, slot, source, away, o).wait_send()
                elif away != 0:
                    @pl.when(sends_row(slot, away) if o == 0 else takes_row(slot, away))
                    def _():
                        t_copy(r, slot, source, away, o).wait_send()

    for i in (0, 1):
        @pl.when(reachable(i))
        def _():
            for r in range(1, rounds, 2):
                over_chunks(lambda c: w_copy(r, c, i).wait_send())

    @pl.when(gives_head)
    def _():
        for r in range(1, rounds, 2):
            head_copy(r).wait_send()

    over_chunks(lambda c: store(c).wait())


def solution(mesh):
    count, peers = mesh.shape["row"], mesh.shape["vec"]

    def per_device(eigvecs, reflectors, factors):
        height, width = eigvecs.shape
        rounds = reflectors.shape[0]
        nb = factors.shape[3]
        groups = height // (2 * nb)
        wide = width // CHUNKS
        f32, bf16, dma = jnp.float32, jnp.bfloat16, pltpu.SemaphoreType.DMA
        links = (rounds // 2, 2, CHUNKS)
        return pl.pallas_call(
            functools.partial(kernel, count, peers),
            out_shape=jax.ShapeDtypeStruct((height, width), f32),
            in_specs=[pl.BlockSpec(memory_space=pltpu.HBM)] * 3,
            out_specs=pl.BlockSpec(memory_space=pl.ANY),
            scratch_shapes=[
                pltpu.VMEM((CHUNKS, height, wide), f32),
                pltpu.VMEM((rounds, nb, height), f32),
                pltpu.VMEM((rounds, groups + 1, nb, nb), f32),
                pltpu.VMEM((rounds, 2 * nb, height), bf16),
                pltpu.VMEM((rounds, height, 3 * nb), bf16),
                pltpu.VMEM(links + (nb, wide), f32),
                pltpu.VMEM(links + (nb, wide), f32),
                dma((CHUNKS,)),
                dma((rounds, 3, peers)),
                dma((rounds, 3, peers)),
                dma((rounds, groups + 1, peers)),
                dma((rounds, groups + 1, peers)),
                dma((rounds,)),
                dma((rounds,)),
                dma(links),
                dma(links),
                dma((CHUNKS,)),
            ],
            compiler_params=pltpu.CompilerParams(
                collective_id=0, has_side_effects=True, vmem_limit_bytes=48 << 20
            ),
            name="back_transform",
        )(
            *(
                pltpu.with_memory_space_constraint(array, pltpu.HBM)
                for array in (eigvecs, jnp.transpose(reflectors, (0, 2, 1)), factors)
            )
        )

    return jax.shard_map(
        per_device,
        mesh=mesh,
        in_specs=(P("row", "vec"), P(None, "row", "vec"), P(None, "row", "vec", None)),
        out_specs=P("row", "vec"),
        check_vma=False,
    )
```
